32 devices in a mesh: seq: 4 (over z), head: 2 (over core), batch: 4 (over y, x).
Axes of the slice: x: 2, y: 2, z: 4, core: 2. Of those that a mesh axis runs over, the one named last changes fastest.
Arguments:
- queries: bfloat16 [16384, 8, 256], P(('batch', 'seq'), 'head'), parts along dimension 0, may hold values from -6 to 6
- keys: bfloat16 [16384, 8, 256], P(('batch', 'seq'), 'head'), parts along dimension 0, may hold values from -0.375 to 0.375
- content_vectors: bfloat16 [16384, 8, 256], P(('batch', 'seq'), 'head'), parts along dimension 0, may hold values from -6 to 6
- decay_rate: float32 [8, 16384], P('head', ('batch', 'seq')), parts along dimension 1, may hold values from 0 to 3
- gate_pre: bfloat16 [16384, 2048], P(('batch', 'seq'), 'head'), parts along dimension 0, may hold values from -6 to 6
- norm_gain: float32 [2048], P('head'), may hold values from 0.1 to 1.9
- out_weight: bfloat16 [2048, 4096], P('head'), may hold values from -0.125 to 0.125
Outputs:
- layer_out: bfloat16 [16384, 4096], P(('batch', 'seq'), 'head'), parts along dimension 0
The draws below stay inside these ranges and needn't reach their ends.
There are 4 independent parts, one for each index of `batch`. The reference program is written for one: setup_inputs(seed, part) draws one part's arguments, and reference() takes and returns one part's arrays. A program takes and returns all parts, laid end to end along the dimension named above; an argument that names none is the same for every part. Nothing has to cross between parts.
All inputs are finite; a program needn't handle non-finite values.
Results may differ from the reference program's by a relative error of at most 0.013.
Values may be sent and summed in bfloat16 or wider, within the bound.
A program may use at most 128 MiB of HBM per device.

```python
import math
import jax
import jax.numpy as jnp
from jax import lax

D = 4096
HEADS = 8
DK = 256
VH = 256
TOK_DEV = 1024
TOKENS = 4096
N_SEQ = 4


def draw_decay_rate(key, part):
    keys_list = jax.random.split(jax.random.fold_in(key, 17), 7)
    ranking = jax.random.permutation(keys_list[0], HEADS)
    sluggish_tally = HEADS // 2
    is_slow = ranking < sluggish_tally
    fast_rate = jnp.exp(jax.random.uniform(keys_list[1], (HEADS,), jnp.float32, math.log(1.0 / 50.0), math.log(1.0 / 30.0)))
    slow_rate = jnp.exp(jax.random.uniform(keys_list[2], (HEADS,), jnp.float32, math.log(0.3 / TOKENS), math.log(0.6 / TOKENS)))
    baseline_decay = jnp.where(is_slow, slow_rate, fast_rate)
    segments = 2 * (TOKENS // TOK_DEV)
    gate_modulation = jnp.exp(jax.random.uniform(keys_list[3], (HEADS, segments), jnp.float32, -0.7, 0.7))
    gate_modulation = jnp.repeat(gate_modulation, TOK_DEV // 2, axis=1)
    noise_level = jax.random.uniform(keys_list[4], (HEADS, TOKENS), jnp.float32, 0.5, 1.5)
    destination_indices = jax.random.randint(keys_list[5], (HEADS, 3), 0, TOKENS)
    loss_values = jax.random.uniform(keys_list[6], (HEADS, 3), jnp.float32, -math.log(0.8), -math.log(0.5))
    token_positions = jnp.arange(TOKENS)
    spike_events = jnp.sum(jnp.where(token_positions[None, None, :] == destination_indices[:, :, None], loss_values[:, :, None], 0.0), axis=1)
    return (baseline_decay[:, None] * gate_modulation * noise_level + spike_events).astype(jnp.float32)


def level_of(rng, dims, shards, smallest, largest):
    loudness, own = 1.0, jax.random.fold_in(rng, 6)
    for position, blocks in shards:
        steps = jnp.exp(jax.random.uniform(jax.random.fold_in(own, position), (blocks,), jnp.float32, smallest / len(shards), largest / len(shards)))
        loudness = loudness * jnp.repeat(steps, dims[position] // blocks).reshape([-1 if axis == position else 1 for axis in range(len(dims))])
    return loudness


def bell_draw(stream_key, dims, scale, reach, pieces=(), dtype=jnp.bfloat16):
    array = jax.random.normal(stream_key, dims, jnp.float32) * scale
    if len(pieces) > 0:
        array = level_of(stream_key, dims, pieces, -0.22, 0.18) * array
    return jnp.clip(array, min=-reach, max=reach).astype(dtype)


def setup_inputs(seed: int = 0, part: int = 0) -> dict:
    seeds = jax.random.split(jax.random.key(seed), 8)
    own_keys = jax.random.split(jax.random.fold_in(seeds[7], part), 8)
    return {
        "queries": bell_draw(own_keys[0], (TOKENS, HEADS, DK), 1.0, 6.0, ((0, 4), (1, 2))),
        "keys": bell_draw(own_keys[1], (TOKENS, HEADS, DK), 0.0625, 0.375, ((0, 4), (1, 2))),
        "content_vectors": bell_draw(own_keys[2], (TOKENS, HEADS, VH), 1.0, 6.0, ((0, 4), (1, 2))),
        "decay_rate": draw_decay_rate(jax.random.fold_in(jax.random.fold_in(seeds[7], part), 71), part),
        "gate_pre": bell_draw(own_keys[4], (TOKENS, HEADS * VH), 1.0, 6.0, ((0, 4), (1, 2))),
        "norm_gain": jnp.clip(1.0 + 0.18 * jax.random.normal(seeds[5], (HEADS * VH,), jnp.float32), 0.1, 1.9),
        "out_weight": bell_draw(seeds[6], (HEADS * VH, D), (HEADS * VH) ** -0.5, 0.125, ((0, 2),)),
    }


def reference(queries, keys, content_vectors, decay_rate, gate_pre, norm_gain, out_weight):
    block_queries = queries.reshape(N_SEQ, TOK_DEV, HEADS, DK)
    block_keys = keys.reshape(N_SEQ, TOK_DEV, HEADS, DK)
    block_values = content_vectors.reshape(N_SEQ, TOK_DEV, HEADS, VH)
    block_rates = decay_rate.reshape(HEADS, N_SEQ, TOK_DEV).transpose(1, 0, 2)
    block_gates = gate_pre.reshape(N_SEQ, TOK_DEV, HEADS * VH)
    token_positions = jnp.arange(TOK_DEV)
    causal = token_positions[:, None] >= token_positions[None, :]

    def one_block(carried_state, inputs):
        current_query_rows, step_keys, present_content_vectors, step_rates, step_gates = inputs
        within = -jnp.cumsum(step_rates, axis=1)
        totals = within[:, -1]
        lookup_vectors_weighted = (jnp.exp(totals[None, :] - within.T)[:, :, None] * step_keys.astype(jnp.float32)).astype(jnp.bfloat16)
        segment_retained_matrix = jnp.einsum('gdj,gdl->djl', lookup_vectors_weighted.astype(jnp.float32), present_content_vectors.astype(jnp.float32))
        arriving_state = carried_state.astype(jnp.bfloat16)
        passed_forward = jnp.einsum('qaw,awi->qai', current_query_rows.astype(jnp.float32), arriving_state.astype(jnp.float32))
        passed_forward = passed_forward * jnp.exp(within.T)[:, :, None]
        scores = jnp.einsum('lhk,shk->hls', current_query_rows.astype(jnp.float32), step_keys.astype(jnp.float32))
        exponent = jnp.where(causal[None], within[:, :, None] - within[:, None, :], -jnp.inf)
        weights = (scores * jnp.exp(exponent)).astype(jnp.bfloat16)
        within_block = jnp.einsum('hls,shv->lhv', weights.astype(jnp.float32), present_content_vectors.astype(jnp.float32))
        retained = passed_forward + within_block
        center = lax.optimization_barrier(jnp.mean(retained, axis=2, keepdims=True))
        shifted = retained - center
        variance = lax.optimization_barrier(jnp.mean(shifted * shifted, axis=2, keepdims=True))
        normed = (shifted * lax.rsqrt(variance + 1e-06)).reshape(TOK_DEV, HEADS * VH)
        gated_rows = (normed * norm_gain * jax.nn.silu(step_gates.astype(jnp.float32))).astype(jnp.bfloat16)
        projected = jnp.dot(gated_rows, out_weight, preferred_element_type=jnp.float32).astype(jnp.bfloat16)
        next_state = jnp.exp(totals)[:, None, None] * carried_state + segment_retained_matrix
        return (next_state, projected)
    start_state = jnp.zeros((HEADS, DK, VH), jnp.float32)
    final_state, outputs = lax.scan(one_block, start_state, (block_queries, block_keys, block_values, block_rates, block_gates))
    return outputs.reshape(TOKENS, D)
```

```python
import functools

import jax
import jax.numpy as jnp
from jax import lax
from jax.experimental import pallas as pl
from jax.experimental.pallas import tpu as pltpu
from jax.sharding import PartitionSpec as P

MESH = pl.DeviceIdType.MESH
SUB = 4
AHEAD = 6
LAG = 2 * SUB + 1


def kernel(
    blocks, q_hbm, k_hbm, v_hbm, rate_ref, gate_hbm, gain_ref, w_hbm, out_hbm,
    qv, kv, vv, gv, w_own, w_peer, g_own, g_peer, acc, ob, near, st, inc, sb,
    wrow, wcol, ecol, fstart, ftot,
    k_sem, v_sem, q_sem, gate_sem, w_sem, ws_sem, wr_sem, ss_sem, sr_sem, gs_sem, gr_sem, o_sem,
):
    length, dk = qv.shape[0], inc.shape[1]
    dv = inc.shape[2]
    heads = inc.shape[0]
    rows = length // SUB
    part = dk // SUB
    half = w_own.shape[1]
    tiles, _, width = acc.shape
    per = tiles // SUB
    s = lax.axis_index("seq")
    p = lax.axis_index("head")

    def k_copy(h):
        c = pl.ds(h * dk, dk)
        return pltpu.make_async_copy(k_hbm.at[:, c], kv.at[:, c], k_sem.at[h])

    def v_copy(h):
        c = pl.ds(h * dv, dv)
        return pltpu.make_async_copy(v_hbm.at[:, c], vv.at[:, c], v_sem.at[h])

    def w_local():
        c = pl.ds(pl.multiple_of(p * half, 128), half)
        return pltpu.make_async_copy(w_hbm.at[:, c], w_own, w_sem)

    def w_remote():
        c = pl.ds(pl.multiple_of((1 - p) * half, 128), half)
        return pltpu.make_async_remote_copy(
            w_hbm.at[:, c], w_peer, ws_sem, wr_sem,
            device_id={"head": 1 - p}, device_id_type=MESH,
        )

    def state_copy(h, j):
        c = pl.ds(pl.multiple_of(j * part, part), part)
        i = h * SUB + j
        return pltpu.make_async_remote_copy(
            sb.at[h, c], inc.at[h, c], ss_sem.at[i], sr_sem.at[i],
            device_id={"seq": lax.rem(s + 1, blocks)}, device_id_type=MESH,
        )

    def g_copy(h, r):
        c = pl.ds(pl.multiple_of(r * rows, rows), rows)
        i = h * SUB + r
        return pltpu.make_async_remote_copy(
            g_own.at[h, c], g_peer.at[h, c], gs_sem.at[i], gr_sem.at[i],
            device_id={"head": 1 - p}, device_id_type=MESH,
        )

    def out_copy(n):
        c = pl.ds(pl.multiple_of(n * width, width), width)
        return pltpu.make_async_copy(ob.at[n], out_hbm.at[:, c], o_sem.at[n])

    for h in range(heads):
        k_copy(h).start()
        v_copy(h).start()
    q_copy = pltpu.make_async_copy(q_hbm, qv, q_sem)
    gate_copy = pltpu.make_async_copy(gate_hbm, gv, gate_sem)
    q_copy.start()
    gate_copy.start()
    w_local().start()

    barrier = pltpu.get_barrier_semaphore()
    for there in (
        {"seq": lax.rem(s + 1, blocks)},
        {"seq": lax.rem(s + blocks - 1, blocks)},
        {"head": 1 - p},
    ):
        pl.semaphore_signal(barrier, inc=1, device_id=there, device_id_type=MESH)

    run = rate_ref[...]
    run = jnp.concatenate([run, run], axis=0)
    lane = lax.broadcasted_iota(jnp.int32, run.shape, 1)
    shift = 1
    while shift < length:
        run = run + jnp.where(lane >= shift, pltpu.roll(run, shift, 1), 0.0)
        shift *= 2
    within = -run
    columns = within.T
    for h in range(heads):
        wrow[h] = within[h : h + 1]
        wcol[h] = columns[:, h : h + 1]

    pl.semaphore_wait(barrier, 3)
    w_remote().start()

    @pl.when(s == 0)
    def _():
        inc[...] = jnp.zeros_like(inc)

    for h in range(heads):
        k_copy(h).wait()
        v_copy(h).wait()
        state = jnp.zeros((dk, dv), jnp.float32)
        start = jnp.zeros((1, 1), jnp.float32)
        for r in range(SUB):
            t = slice(r * rows, (r + 1) * rows)
            w = columns[t, h : h + 1]
            end = within[h : h + 1, (r + 1) * rows - 1 : (r + 1) * rows]
            ecol[h, t] = jnp.exp(w - start)
            fstart[h * SUB + r] = jnp.broadcast_to(jnp.exp(start), (1, dv))
            st[h * (SUB + 1) + r] = state
            scaled = (jnp.exp(end - w) * kv[t, h * dk : (h + 1) * dk]).astype(jnp.bfloat16)
            added = lax.dot_general(
                scaled, vv[t, h * dv : (h + 1) * dv], (((0,), (0,)), ((), ())),
                preferred_element_type=jnp.float32,
            )
            state = jnp.exp(end - start) * state + added
            start = end
        ftot[h] = jnp.broadcast_to(jnp.exp(start), (1, dv))
        st[h * (SUB + 1) + SUB] = state

        @pl.when(s == 0)
        def _():
            sb[h] = state.astype(jnp.bfloat16)
            for j in range(SUB):
                state_copy(h, j).start()

    q_copy.wait()
    gate_copy.wait()
    steps = heads * SUB
    lead = jnp.minimum(AHEAD * s, steps)

    def step(i, carry):
        @pl.when(i < steps)
        def _():
            h, r = i // SUB, lax.rem(i, SUB)
            t = pl.ds(pl.multiple_of(r * rows, rows), rows)
            ck = pl.ds(pl.multiple_of(h * dk, dk), dk)
            cv = pl.ds(pl.multiple_of(h * dv, dv), dv)
            scores = lax.dot_general(
                qv[t, ck], kv[t, ck], (((1,), (1,)), ((), ())), preferred_element_type=jnp.float32
            )
            y = lax.broadcasted_iota(jnp.int32, (rows, rows), 0)
            x = lax.broadcasted_iota(jnp.int32, (rows, rows), 1)
            gap = jnp.where(y >= x, wcol[h, t] - wrow[h, :, t], -jnp.inf)
            weights = (scores * jnp.exp(gap)).astype(jnp.bfloat16)
            near[h, t] = jnp.dot(weights, vv[t, cv], preferred_element_type=jnp.float32)

        c = i - lead

        @pl.when((c >= 0) & (c < steps) & (s > 0))
        def _():
            h, j = c // SUB, lax.rem(c, SUB)
            state_copy(h, j).wait_recv()

            @pl.when(s < blocks - 1)
            def _():
                t = pl.ds(pl.multiple_of(j * part, part), part)
                total = ftot[h] * inc[h, t].astype(jnp.float32) + st[h * (SUB + 1) + SUB, t]
                sb[h, t] = total.astype(jnp.bfloat16)
                state_copy(h, j).start()

        f = c - SUB

        @pl.when((f >= 0) & (f < steps))
        def _():
            h, r = f // SUB, lax.rem(f, SUB)
            t = pl.ds(pl.multiple_of(r * rows, rows), rows)
            ck = pl.ds(pl.multiple_of(h * dk, dk), dk)
            cv = pl.ds(pl.multiple_of(h * dv, dv), dv)
            state = st[h * (SUB + 1) + r] + fstart[h * SUB + r] * inc[h].astype(jnp.float32)
            far = jnp.dot(
                qv[t, ck], state.astype(jnp.bfloat16), preferred_element_type=jnp.float32
            )
            kept = near[h, t] + ecol[h, t] * far
            kept = kept - jnp.mean(kept, axis=1, keepdims=True)
            var = jnp.mean(kept * kept, axis=1, keepdims=True)
            g = gv[t, cv].astype(jnp.float32)
            gated = kept * lax.rsqrt(var + 1e-06) * gain_ref[:, cv] * (g / (1.0 + jnp.exp(-g)))
            g_own[h, t] = gated.astype(jnp.bfloat16)
            g_copy(h, r).start()

        o = c - LAG

        @pl.when(o == 0)
        def _():
            w_local().wait()
            w_remote().wait_recv()

        @pl.when((o >= 0) & (lax.rem(o, SUB) == 0))
        def _():
            for r in range(SUB):
                g_copy(o // SUB, r).wait_recv()

        @pl.when(o >= 0)
        def _():
            h = o // SUB
            ch = pl.ds(pl.multiple_of(h * dv, dv), dv)
            for u in range(per):
                n = lax.rem(o, SUB) * per + u
                cn = pl.ds(pl.multiple_of(n * width, width), width)
                total = jnp.dot(g_own[h], w_own[ch, cn], preferred_element_type=jnp.float32)
                total += jnp.dot(g_peer[h], w_peer[ch, cn], preferred_element_type=jnp.float32)

                @pl.when(h == 0)
                def _():
                    acc[n] = total

                @pl.when((h > 0) & (h < heads - 1))
                def _():
                    acc[n] += total

                @pl.when(h == heads - 1)
                def _():
                    ob[n] = (acc[n] + total).astype(jnp.bfloat16)
                    out_copy(n).start()

        return carry

    lax.fori_loop(0, lead + steps + LAG, step, 0)

    w_remote().wait_send()

    def finish(i, carry):
        g_copy(i // SUB, lax.rem(i, SUB)).wait_send()

        @pl.when(s < blocks - 1)
        def _():
            state_copy(i // SUB, lax.rem(i, SUB)).wait_send()

        return carry

    lax.fori_loop(0, steps, finish, 0)
    for n in range(tiles):
        out_copy(n).wait()


def on_device(queries, keys, content_vectors, decay_rate, gate_pre, norm_gain, out_weight):
    length, heads, dk = queries.shape
    dv = content_vectors.shape[2]
    blocks = lax.axis_size("seq")
    half = out_weight.shape[1] // lax.axis_size("head")
    tiles = 2 * SUB
    width = half // tiles
    rows = heads * dv
    anywhere = pl.BlockSpec(memory_space=pl.ANY)
    vmem = pl.BlockSpec(memory_space=pltpu.VMEM)
    steps = heads * SUB
    bf16, f32 = jnp.bfloat16, jnp.float32
    dma = pltpu.SemaphoreType.DMA
    return pl.pallas_call(
        functools.partial(kernel, blocks),
        out_shape=jax.ShapeDtypeStruct((length, half), bf16),
        in_specs=[anywhere, anywhere, anywhere, vmem, anywhere, vmem, anywhere],
        out_specs=anywhere,
        scratch_shapes=[
            pltpu.VMEM((length, heads * dk), bf16),
            pltpu.VMEM((length, heads * dk), bf16),
            pltpu.VMEM((length, rows), bf16),
            pltpu.VMEM((length, rows), bf16),
            pltpu.VMEM((rows, half), bf16),
            pltpu.VMEM((rows, half), bf16),
            pltpu.VMEM((heads, length, dv), bf16),
            pltpu.VMEM((heads, length, dv), bf16),
            pltpu.VMEM((tiles, length, width), f32),
            pltpu.VMEM((tiles, length, width), bf16),
            pltpu.VMEM((heads, length, dv), f32),
            pltpu.VMEM((heads * (SUB + 1), dk, dv), f32),
            pltpu.VMEM((heads, dk, dv), bf16),
            pltpu.VMEM((heads, dk, dv), bf16),
            pltpu.VMEM((heads, 1, length), f32),
            pltpu.VMEM((heads, length, 1), f32),
            pltpu.VMEM((heads, length, 1), f32),
            pltpu.VMEM((steps, 1, dv), f32),
            pltpu.VMEM((heads, 1, dv), f32),
            dma((heads,)), dma((heads,)), dma, dma, dma, dma, dma,
            dma((steps,)), dma((steps,)), dma((steps,)), dma((steps,)), dma((tiles,)),
        ],
        compiler_params=pltpu.CompilerParams(
            collective_id=0, has_side_effects=True, vmem_limit_bytes=64000 * 1024
        ),
    )(
        queries.reshape(length, heads * dk),
        keys.reshape(length, heads * dk),
        content_vectors.reshape(length, rows),
        decay_rate,
        gate_pre,
        norm_gain.reshape(1, rows),
        out_weight,
    )


def solution(mesh):
    in_specs = (
        P(("batch", "seq"), "head", None),
        P(("batch", "seq"), "head", None),
        P(("batch", "seq"), "head", None),
        P("head", ("batch", "seq")),
        P(("batch", "seq"), "head"),
        P("head"),
        P("head", None),
    )
    out_specs = P(("batch", "seq"), "head")
    return jax.shard_map(
        on_device, mesh=mesh, in_specs=in_specs, out_specs=out_specs, check_vma=False
    )
```

```python
import functools

import jax
import jax.numpy as jnp
from jax import lax
from jax.experimental import pallas as pl
from jax.experimental.pallas import tpu as pltpu
from jax.sharding import PartitionSpec as P

MESH = pl.DeviceIdType.MESH
SUB = 4
AHEAD = 6
GROUPS = 2


def kernel(
    blocks, q_hbm, k_hbm, v_hbm, rate_ref, gate_hbm, gain_ref, w_hbm, out_hbm,
    qv, kv, vv, gv, w_all, g_all, acc, ob, near, st, inc, sb,
    wrow, wcol, ecol, fstart, ftot,
    k_sem, v_sem, q_sem, gate_sem, w_sem, ws_sem, wr_sem, ss_sem, sr_sem, gs_sem, gr_sem, o_sem,
):
    length, dk = qv.shape[0], inc.shape[1]
    dv = inc.shape[2]
    heads = inc.shape[0]
    rows = length // SUB
    part = dk // SUB
    half = w_all.shape[2]
    fold = heads // GROUPS
    deep = fold * dv
    tiles, _, width = acc.shape
    lag = SUB * (fold + 1) + 1
    s = lax.axis_index("seq")
    p = lax.axis_index("head")

    def k_copy(h):
        c = pl.ds(h * dk, dk)
        return pltpu.make_async_copy(k_hbm.at[:, c], kv.at[:, c], k_sem.at[h])

    def v_copy(h):
        c = pl.ds(h * dv, dv)
        return pltpu.make_async_copy(v_hbm.at[:, c], vv.at[:, c], v_sem.at[h])

    def w_local(g):
        c = pl.ds(pl.multiple_of(p * half, 128), half)
        return pltpu.make_async_copy(
            w_hbm.at[pl.ds(g * deep, deep), c], w_all.at[g, pl.ds(0, deep)], w_sem.at[g]
        )

    def w_remote(g):
        c = pl.ds(pl.multiple_of((1 - p) * half, 128), half)
        return pltpu.make_async_remote_copy(
            w_hbm.at[pl.ds(g * deep, deep), c], w_all.at[g, pl.ds(deep, deep)],
            ws_sem.at[g], wr_sem.at[g],
            device_id={"head": 1 - p}, device_id_type=MESH,
        )

    def state_copy(h, j):
        c = pl.ds(pl.multiple_of(j * part, part), part)
        i = h * SUB + j
        return pltpu.make_async_remote_copy(
            sb.at[h, c], inc.at[h, c], ss_sem.at[i], sr_sem.at[i],
            device_id={"seq": lax.rem(s + 1, blocks)}, device_id_type=MESH,
        )

    def g_copy(h, r):
        c = pl.ds(pl.multiple_of(r * rows, rows), rows)
        i = h * SUB + r
        g, m = h // fold, lax.rem(h, fold)
        here = pl.ds(pl.multiple_of(m * dv, dv), dv)
        there = pl.ds(pl.multiple_of(deep + m * dv, dv), dv)
        return pltpu.make_async_remote_copy(
            g_all.at[g, c, here], g_all.at[g, c, there], gs_sem.at[i], gr_sem.at[i],
            device_id={"head": 1 - p}, device_id_type=MESH,
        )

    def out_copy(n):
        c = pl.ds(pl.multiple_of(n * width, width), width)
        return pltpu.make_async_copy(ob.at[n], out_hbm.at[:, c], o_sem.at[n])

    for h in range(heads):
        k_copy(h).start()
        v_copy(h).start()
    q_copy = pltpu.make_async_copy(q_hbm, qv, q_sem)
    gate_copy = pltpu.make_async_copy(gate_hbm, gv, gate_sem)
    q_copy.start()
    gate_copy.start()
    for g in range(GROUPS):
        w_local(g).start()

    barrier = pltpu.get_barrier_semaphore()
    for there in (
        {"seq": lax.rem(s + 1, blocks)},
        {"seq": lax.rem(s + blocks - 1, blocks)},
        {"head": 1 - p},
    ):
        pl.semaphore_signal(barrier, inc=1, device_id=there, device_id_type=MESH)

    run = rate_ref[...]
    run = jnp.concatenate([run, run], axis=0)
    lane = lax.broadcasted_iota(jnp.int32, run.shape, 1)
    shift = 1
    while shift < length:
        run = run + jnp.where(lane >= shift, pltpu.roll(run, shift, 1), 0.0)
        shift *= 2
    within = -run
    columns = within.T
    for h in range(heads):
        wrow[h] = within[h : h + 1]
        wcol[h] = columns[:, h : h + 1]

    pl.semaphore_wait(barrier, 3)
    for g in range(GROUPS):
        w_remote(g).start()

    @pl.when(s == 0)
    def _():
        inc[...] = jnp.zeros_like(inc)

    for h in range(heads):
        k_copy(h).wait()
        v_copy(h).wait()
        state = jnp.zeros((dk, dv), jnp.float32)
        start = jnp.zeros((1, 1), jnp.float32)
        for r in range(SUB):
            t = slice(r * rows, (r + 1) * rows)
            w = columns[t, h : h + 1]
            end = within[h : h + 1, (r + 1) * rows - 1 : (r + 1) * rows]
            ecol[h, t] = jnp.exp(w - start)
            fstart[h * SUB + r] = jnp.broadcast_to(jnp.exp(start), (1, dv))
            st[h * (SUB + 1) + r] = state
            scaled = (jnp.exp(end - w) * kv[t, h * dk : (h + 1) * dk]).astype(jnp.bfloat16)
            added = lax.dot_general(
                scaled, vv[t, h * dv : (h + 1) * dv], (((0,), (0,)), ((), ())),
                preferred_element_type=jnp.float32,
            )
            state = jnp.exp(end - start) * state + added
            start = end
        ftot[h] = jnp.broadcast_to(jnp.exp(start), (1, dv))
        st[h * (SUB + 1) + SUB] = state

        @pl.when(s == 0)
        def _():
            sb[h] = state.astype(jnp.bfloat16)
            for j in range(SUB):
                state_copy(h, j).start()

    q_copy.wait()
    gate_copy.wait()
    steps = heads * SUB
    lead = jnp.minimum(AHEAD * s, steps)

    def step(i, carry):
        @pl.when(i < steps)
        def _():
            h, r = i // SUB, lax.rem(i, SUB)
            t = pl.ds(pl.multiple_of(r * rows, rows), rows)
            ck = pl.ds(pl.multiple_of(h * dk, dk), dk)
            cv = pl.ds(pl.multiple_of(h * dv, dv), dv)
            scores = lax.dot_general(
                qv[t, ck], kv[t, ck], (((1,), (1,)), ((), ())), preferred_element_type=jnp.float32
            )
            y = lax.broadcasted_iota(jnp.int32, (rows, rows), 0)
            x = lax.broadcasted_iota(jnp.int32, (rows, rows), 1)
            gap = jnp.where(y >= x, wcol[h, t] - wrow[h, :, t], -jnp.inf)
            weights = (scores * jnp.exp(gap)).astype(jnp.bfloat16)
            near[h, t] = jnp.dot(weights, vv[t, cv], preferred_element_type=jnp.float32)

        c = i - lead

        @pl.when((c >= 0) & (c < steps) & (s > 0))
        def _():
            h, j = c // SUB, lax.rem(c, SUB)
            state_copy(h, j).wait_recv()

            @pl.when(s < blocks - 1)
            def _():
                t = pl.ds(pl.multiple_of(j * part, part), part)
                total = ftot[h] * inc[h, t].astype(jnp.float32) + st[h * (SUB + 1) + SUB, t]
                sb[h, t] = total.astype(jnp.bfloat16)
                state_copy(h, j).start()

        f = c - SUB

        @pl.when((f >= 0) & (f < steps))
        def _():
            h, r = f // SUB, lax.rem(f, SUB)
            t = pl.ds(pl.multiple_of(r * rows, rows), rows)
            ck = pl.ds(pl.multiple_of(h * dk, dk), dk)
            cv = pl.ds(pl.multiple_of(h * dv, dv), dv)
            state = st[h * (SUB + 1) + r] + fstart[h * SUB + r] * inc[h].astype(jnp.float32)
            far = jnp.dot(
                qv[t, ck], state.astype(jnp.bfloat16), preferred_element_type=jnp.float32
            )
            kept = near[h, t] + ecol[h, t] * far
            kept = kept - jnp.mean(kept, axis=1, keepdims=True)
            var = jnp.mean(kept * kept, axis=1, keepdims=True)
            g = gv[t, cv].astype(jnp.float32)
            gated = kept * lax.rsqrt(var + 1e-06) * gain_ref[:, cv] * (g / (1.0 + jnp.exp(-g)))
            here = pl.ds(pl.multiple_of(lax.rem(h, fold) * dv, dv), dv)
            g_all[h // fold, t, here] = gated.astype(jnp.bfloat16)
            g_copy(h, r).start()

        o = c - lag

        for g in range(GROUPS):

            @pl.when(o == g * tiles)
            def _():
                w_local(g).wait()
                w_remote(g).wait_recv()
                for m in range(fold):
                    for r in range(SUB):
                        g_copy(g * fold + m, r).wait_recv()

            @pl.when((o >= g * tiles) & (o < (g + 1) * tiles))
            def _():
                n = o - g * tiles
                cn = pl.ds(pl.multiple_of(n * width, width), width)
                total = jnp.dot(g_all[g], w_all[g, :, cn], preferred_element_type=jnp.float32)
                if g > 0:
                    total += acc[n]
                if g < GROUPS - 1:
                    acc[n] = total
                else:
                    ob[n] = total.astype(jnp.bfloat16)
                    out_copy(n).start()

        return carry

    lax.fori_loop(0, lead + lag + GROUPS * tiles, step, 0)

    for g in range(GROUPS):
        w_remote(g).wait_send()

    def finish(i, carry):
        g_copy(i // SUB, lax.rem(i, SUB)).wait_send()

        @pl.when(s < blocks - 1)
        def _():
            state_copy(i // SUB, lax.rem(i, SUB)).wait_send()

        return carry

    lax.fori_loop(0, steps, finish, 0)
    for n in range(tiles):
        out_copy(n).wait()


def on_device(queries, keys, content_vectors, decay_rate, gate_pre, norm_gain, out_weight):
    length, heads, dk = queries.shape
    dv = content_vectors.shape[2]
    blocks = lax.axis_size("seq")
    half = out_weight.shape[1] // lax.axis_size("head")
    tiles = 2 * SUB
    width = half // tiles
    rows = heads * dv
    anywhere = pl.BlockSpec(memory_space=pl.ANY)
    vmem = pl.BlockSpec(memory_space=pltpu.VMEM)
    steps = heads * SUB
    bf16, f32 = jnp.bfloat16, jnp.float32
    dma = pltpu.SemaphoreType.DMA
    return pl.pallas_call(
        functools.partial(kernel, blocks),
        out_shape=jax.ShapeDtypeStruct((length, half), bf16),
        in_specs=[anywhere, anywhere, anywhere, vmem, anywhere, vmem, anywhere],
        out_specs=anywhere,
        scratch_shapes=[
            pltpu.VMEM((length, heads * dk), bf16),
            pltpu.VMEM((length, heads * dk), bf16),
            pltpu.VMEM((length, rows), bf16),
            pltpu.VMEM((length, rows), bf16),
            pltpu.VMEM((GROUPS, 2 * rows // GROUPS, half), bf16),
            pltpu.VMEM((GROUPS, length, 2 * rows // GROUPS), bf16),
            pltpu.VMEM((tiles, length, width), f32),
            pltpu.VMEM((tiles, length, width), bf16),
            pltpu.VMEM((heads, length, dv), f32),
            pltpu.VMEM((heads * (SUB + 1), dk, dv), f32),
            pltpu.VMEM((heads, dk, dv), bf16),
            pltpu.VMEM((heads, dk, dv), bf16),
            pltpu.VMEM((heads, 1, length), f32),
            pltpu.VMEM((heads, length, 1), f32),
            pltpu.VMEM((heads, length, 1), f32),
            pltpu.VMEM((steps, 1, dv), f32),
            pltpu.VMEM((heads, 1, dv), f32),
            dma((heads,)), dma((heads,)), dma, dma,
            dma((GROUPS,)), dma((GROUPS,)), dma((GROUPS,)),
            dma((steps,)), dma((steps,)), dma((steps,)), dma((steps,)), dma((tiles,)),
        ],
        compiler_params=pltpu.CompilerParams(
            collective_id=0, has_side_effects=True, vmem_limit_bytes=64000 * 1024
        ),
    )(
        queries.reshape(length, heads * dk),
        keys.reshape(length, heads * dk),
        content_vectors.reshape(length, rows),
        decay_rate,
        gate_pre,
        norm_gain.reshape(1, rows),
        out_weight,
    )


def solution(mesh):
    in_specs = (
        P(("batch", "seq"), "head", None),
        P(("batch", "seq"), "head", None),
        P(("batch", "seq"), "head", None),
        P("head", ("batch", "seq")),
        P(("batch", "seq"), "head"),
        P("head"),
        P("head", None),
    )
    out_specs = P(("batch", "seq"), "head")
    return jax.shard_map(
        on_device, mesh=mesh, in_specs=in_specs, out_specs=out_specs, check_vma=False
    )
```

```python
import functools

import jax
import jax.numpy as jnp
from jax import lax
from jax.experimental import pallas as pl
from jax.experimental.pallas import tpu as pltpu
from jax.sharding import PartitionSpec as P

MESH = pl.DeviceIdType.MESH
SUB = 4
AHEAD = 6
GROUPS = 2


def kernel(
    blocks, q_hbm, k_hbm, v_hbm, rate_ref, gate_hbm, gain_ref, w_hbm, out_hbm,
    q_raw, k_raw, v_raw, qv, kv, vv, gv, w_all, g_all, acc, ob, near, st, inc, sb,
    wrow, wcol, ecol, fstart, ftot,
    k_sem, v_sem, q_sem, gate_sem, w_sem, ws_sem, wr_sem, ss_sem, sr_sem, gs_sem, gr_sem, o_sem,
):
    length, dk = qv.shape[0], inc.shape[1]
    dv = inc.shape[2]
    heads = inc.shape[0]
    rows = length // SUB
    part = dk // SUB
    half = w_all.shape[2]
    fold = heads // GROUPS
    deep = fold * dv
    tiles, _, width = acc.shape
    lag = SUB * (fold + 1) + 1
    s = lax.axis_index("seq")
    p = lax.axis_index("head")

    k_copy = pltpu.make_async_copy(k_hbm, k_raw, k_sem)
    v_copy = pltpu.make_async_copy(v_hbm, v_raw, v_sem)

    def flatten(raw, flat):
        fine = rows // SUB

        def piece(i, carry):
            t = pl.ds(pl.multiple_of(i * fine, fine), fine)
            flat[t] = raw[t].reshape(fine, flat.shape[1])
            return carry

        lax.fori_loop(0, length // fine, piece, 0)

    def w_local(g):
        c = pl.ds(pl.multiple_of(p * half, 128), half)
        return pltpu.make_async_copy(
            w_hbm.at[pl.ds(g * deep, deep), c], w_all.at[g, pl.ds(0, deep)], w_sem.at[g]
        )

    def w_remote(g):
        c = pl.ds(pl.multiple_of((1 - p) * half, 128), half)
        return pltpu.make_async_remote_copy(
            w_hbm.at[pl.ds(g * deep, deep), c], w_all.at[g, pl.ds(deep, deep)],
            ws_sem.at[g], wr_sem.at[g],
            device_id={"head": 1 - p}, device_id_type=MESH,
        )

    def state_copy(h, j):
        c = pl.ds(pl.multiple_of(j * part, part), part)
        i = h * SUB + j
        return pltpu.make_async_remote_copy(
            sb.at[h, c], inc.at[h, c], ss_sem.at[i], sr_sem.at[i],
            device_id={"seq": lax.rem(s + 1, blocks)}, device_id_type=MESH,
        )

    def g_copy(h, r):
        c = pl.ds(pl.multiple_of(r * rows, rows), rows)
        i = h * SUB + r
        g, m = h // fold, lax.rem(h, fold)
        here = pl.ds(pl.multiple_of(m * dv, dv), dv)
        there = pl.ds(pl.multiple_of(deep + m * dv, dv), dv)
        return pltpu.make_async_remote_copy(
            g_all.at[g, c, here], g_all.at[g, c, there], gs_sem.at[i], gr_sem.at[i],
            device_id={"head": 1 - p}, device_id_type=MESH,
        )

    def out_copy(n):
        c = pl.ds(pl.multiple_of(n * width, width), width)
        return pltpu.make_async_copy(ob.at[n], out_hbm.at[:, c], o_sem.at[n])

    k_copy.start()
    v_copy.start()
    q_copy = pltpu.make_async_copy(q_hbm, q_raw, q_sem)
    gate_copy = pltpu.make_async_copy(gate_hbm, gv, gate_sem)
    q_copy.start()
    gate_copy.start()
    for g in range(GROUPS):
        w_local(g).start()

    barrier = pltpu.get_barrier_semaphore()
    for there in (
        {"seq": lax.rem(s + 1, blocks)},
        {"seq": lax.rem(s + blocks - 1, blocks)},
        {"head": 1 - p},
    ):
        pl.semaphore_signal(barrier, inc=1, device_id=there, device_id_type=MESH)

    run = rate_ref[...]
    run = jnp.concatenate([run, run], axis=0)
    lane = lax.broadcasted_iota(jnp.int32, run.shape, 1)
    shift = 1
    while shift < length:
        run = run + jnp.where(lane >= shift, pltpu.roll(run, shift, 1), 0.0)
        shift *= 2
    within = -run
    columns = within.T
    for h in range(heads):
        wrow[h] = within[h : h + 1]
        wcol[h] = columns[:, h : h + 1]

    pl.semaphore_wait(barrier, 3)
    for g in range(GROUPS):
        w_remote(g).start()

    @pl.when(s == 0)
    def _():
        inc[...] = jnp.zeros_like(inc)

    k_copy.wait()
    flatten(k_raw, kv)
    v_copy.wait()
    flatten(v_raw, vv)
    for h in range(heads):
        state = jnp.zeros((dk, dv), jnp.float32)
        start = jnp.zeros((1, 1), jnp.float32)
        for r in range(SUB):
            t = slice(r * rows, (r + 1) * rows)
            w = columns[t, h : h + 1]
            end = within[h : h + 1, (r + 1) * rows - 1 : (r + 1) * rows]
            ecol[h, t] = jnp.exp(w - start)
            fstart[h * SUB + r] = jnp.broadcast_to(jnp.exp(start), (1, dv))
            st[h * (SUB + 1) + r] = state
            scaled = (jnp.exp(end - w) * kv[t, h * dk : (h + 1) * dk]).astype(jnp.bfloat16)
            added = lax.dot_general(
                scaled, vv[t, h * dv : (h + 1) * dv], (((0,), (0,)), ((), ())),
                preferred_element_type=jnp.float32,
            )
            state = jnp.exp(end - start) * state + added
            start = end
        ftot[h] = jnp.broadcast_to(jnp.exp(start), (1, dv))
        st[h * (SUB + 1) + SUB] = state

        @pl.when(s == 0)
        def _():
            sb[h] = state.astype(jnp.bfloat16)
            for j in range(SUB):
                state_copy(h, j).start()

    q_copy.wait()
    flatten(q_raw, qv)
    gate_copy.wait()
    steps = heads * SUB
    lead = jnp.minimum(AHEAD * s, steps)

    def step(i, carry):
        @pl.when(i < steps)
        def _():
            h, r = i // SUB, lax.rem(i, SUB)
            t = pl.ds(pl.multiple_of(r * rows, rows), rows)
            ck = pl.ds(pl.multiple_of(h * dk, dk), dk)
            cv = pl.ds(pl.multiple_of(h * dv, dv), dv)
            scores = lax.dot_general(
                qv[t, ck], kv[t, ck], (((1,), (1,)), ((), ())), preferred_element_type=jnp.float32
            )
            y = lax.broadcasted_iota(jnp.int32, (rows, rows), 0)
            x = lax.broadcasted_iota(jnp.int32, (rows, rows), 1)
            gap = jnp.where(y >= x, wcol[h, t] - wrow[h, :, t], -jnp.inf)
            weights = (scores * jnp.exp(gap)).astype(jnp.bfloat16)
            near[h, t] = jnp.dot(weights, vv[t, cv], preferred_element_type=jnp.float32)

        c = i - lead

        @pl.when((c >= 0) & (c < steps) & (s > 0))
        def _():
            h, j = c // SUB, lax.rem(c, SUB)
            state_copy(h, j).wait_recv()

            @pl.when(s < blocks - 1)
            def _():
                t = pl.ds(pl.multiple_of(j * part, part), part)
                total = ftot[h] * inc[h, t].astype(jnp.float32) + st[h * (SUB + 1) + SUB, t]
                sb[h, t] = total.astype(jnp.bfloat16)
                state_copy(h, j).start()

        f = c - SUB

        @pl.when((f >= 0) & (f < steps))
        def _():
            h, r = f // SUB, lax.rem(f, SUB)
            t = pl.ds(pl.multiple_of(r * rows, rows), rows)
            ck = pl.ds(pl.multiple_of(h * dk, dk), dk)
            cv = pl.ds(pl.multiple_of(h * dv, dv), dv)
            state = st[h * (SUB + 1) + r] + fstart[h * SUB + r] * inc[h].astype(jnp.float32)
            far = jnp.dot(
                qv[t, ck], state.astype(jnp.bfloat16), preferred_element_type=jnp.float32
            )
            kept = near[h, t] + ecol[h, t] * far
            kept = kept - jnp.mean(kept, axis=1, keepdims=True)
            var = jnp.mean(kept * kept, axis=1, keepdims=True)
            g = gv[t, cv].astype(jnp.float32)
            gated = kept * lax.rsqrt(var + 1e-06) * gain_ref[:, cv] * (g / (1.0 + jnp.exp(-g)))
            here = pl.ds(pl.multiple_of(lax.rem(h, fold) * dv, dv), dv)
            g_all[h // fold, t, here] = gated.astype(jnp.bfloat16)
            g_copy(h, r).start()

        o = c - lag

        for g in range(GROUPS):

            @pl.when(o == g * tiles)
            def _():
                w_local(g).wait()
                w_remote(g).wait_recv()
                for m in range(fold):
                    for r in range(SUB):
                        g_copy(g * fold + m, r).wait_recv()

            @pl.when((o >= g * tiles) & (o < (g + 1) * tiles))
            def _():
                n = o - g * tiles
                cn = pl.ds(pl.multiple_of(n * width, width), width)
                total = jnp.dot(g_all[g], w_all[g, :, cn], preferred_element_type=jnp.float32)
                if g > 0:
                    total += acc[n]
                if g < GROUPS - 1:
                    acc[n] = total
                else:
                    ob[n] = total.astype(jnp.bfloat16)
                    out_copy(n).start()

        return carry

    lax.fori_loop(0, lead + lag + GROUPS * tiles, step, 0)

    for g in range(GROUPS):
        w_remote(g).wait_send()

    def finish(i, carry):
        g_copy(i // SUB, lax.rem(i, SUB)).wait_send()

        @pl.when(s < blocks - 1)
        def _():
            state_copy(i // SUB, lax.rem(i, SUB)).wait_send()

        return carry

    lax.fori_loop(0, steps, finish, 0)
    for n in range(tiles):
        out_copy(n).wait()


def on_device(queries, keys, content_vectors, decay_rate, gate_pre, norm_gain, out_weight):
    length, heads, dk = queries.shape
    dv = content_vectors.shape[2]
    blocks = lax.axis_size("seq")
    half = out_weight.shape[1] // lax.axis_size("head")
    tiles = 2 * SUB
    width = half // tiles
    rows = heads * dv
    anywhere = pl.BlockSpec(memory_space=pl.ANY)
    vmem = pl.BlockSpec(memory_space=pltpu.VMEM)
    steps = heads * SUB
    bf16, f32 = jnp.bfloat16, jnp.float32
    dma = pltpu.SemaphoreType.DMA
    return pl.pallas_call(
        functools.partial(kernel, blocks),
        out_shape=jax.ShapeDtypeStruct((length, half), bf16),
        in_specs=[anywhere, anywhere, anywhere, vmem, anywhere, vmem, anywhere],
        out_specs=anywhere,
        scratch_shapes=[
            pltpu.VMEM(queries.shape, bf16),
            pltpu.VMEM(keys.shape, bf16),
            pltpu.VMEM(content_vectors.shape, bf16),
            pltpu.VMEM((length, heads * dk), bf16),
            pltpu.VMEM((length, heads * dk), bf16),
            pltpu.VMEM((length, rows), bf16),
            pltpu.VMEM((length, rows), bf16),
            pltpu.VMEM((GROUPS, 2 * rows // GROUPS, half), bf16),
            pltpu.VMEM((GROUPS, length, 2 * rows // GROUPS), bf16),
            pltpu.VMEM((tiles, length, width), f32),
            pltpu.VMEM((tiles, length, width), bf16),
            pltpu.VMEM((heads, length, dv), f32),
            pltpu.VMEM((heads * (SUB + 1), dk, dv), f32),
            pltpu.VMEM((heads, dk, dv), bf16),
            pltpu.VMEM((heads, dk, dv), bf16),
            pltpu.VMEM((heads, 1, length), f32),
            pltpu.VMEM((heads, length, 1), f32),
            pltpu.VMEM((heads, length, 1), f32),
            pltpu.VMEM((steps, 1, dv), f32),
            pltpu.VMEM((heads, 1, dv), f32),
            dma, dma, dma, dma,
            dma((GROUPS,)), dma((GROUPS,)), dma((GROUPS,)),
            dma((steps,)), dma((steps,)), dma((steps,)), dma((steps,)), dma((tiles,)),
        ],
        compiler_params=pltpu.CompilerParams(
            collective_id=0, has_side_effects=True, vmem_limit_bytes=64000 * 1024
        ),
    )(
        queries,
        keys,
        content_vectors,
        decay_rate,
        gate_pre,
        norm_gain.reshape(1, rows),
        out_weight,
    )


def solution(mesh):
    in_specs = (
        P(("batch", "seq"), "head", None),
        P(("batch", "seq"), "head", None),
        P(("batch", "seq"), "head", None),
        P("head", ("batch", "seq")),
        P(("batch", "seq"), "head"),
        P("head"),
        P("head", None),
    )
    out_specs = P(("batch", "seq"), "head")
    return jax.shard_map(
        on_device, mesh=mesh, in_specs=in_specs, out_specs=out_specs, check_vma=False
    )
```
